128 devices in a mesh: attn: 4 (over z), expert: 32 (over y, x, core).
Axes of the slice: x: 4, y: 4, z: 4, core: 2. Of those that a mesh axis runs over, the one named last changes fastest.
Arguments:
- tokens: bfloat16 [1024, 4096], P(('attn', 'expert')), may hold values from -6 to 6
- expert_ids: int32 [1024, 8], P(('attn', 'expert')), may hold values from 0 to 63, all different within a row; in each aligned block of 8 rows (0 to 7, 8 to 15, ...) at most 3 rows name the same one
- route_gates: bfloat16 [1024, 8], P(('attn', 'expert')), may hold values from 0.049804688 to 0.59765625
- w_gate: bfloat16 [64, 4096, 1536], P('expert', None, 'attn'), may hold values from -0.09375 to 0.09375
- w_up: bfloat16 [64, 4096, 1536], P('expert', None, 'attn'), may hold values from -0.09375 to 0.09375
- w_down: bfloat16 [64, 1536, 4096], P('expert', 'attn'), may hold values from -0.15625 to 0.15625
Outputs:
- mixed: bfloat16 [1024, 4096], P(('attn', 'expert'))
The draws below stay inside these ranges and needn't reach their ends.
Inputs may be any that keep to these rules, and one draw needn't show every extreme that they name: `expert_ids`: A token's 8 ids differ. Within one device's block of 8 tokens no expert is picked more than 3 times, and in every draw some expert is picked exactly 3 times in some block.
All inputs are finite; a program needn't handle non-finite values.
Results may differ from the reference program's by a relative error of at most 0.013.
Values may be sent and summed in bfloat16 or wider, within the bound.
No kernel may reach another device: no remote copies, remote signals or barrier semaphores. Data moves between devices by JAX's collectives and lax.ppermute only.
A program may use at most 128 MiB of HBM per device.

```python
import math
import jax
import jax.numpy as jnp
import numpy as np
from jax import lax

D = 4096
FF = 1536
TOP = 8
TOK_DEV = 8
EXPERTS = 64
TOKENS = 1024
CAP = 3
SLICE = 384
N_ATTN = 4


def block_levels(key, dims, split, low, top_value):
    gain, own = 1.0, jax.random.fold_in(key, 6)
    for dim, parts in split:
        draws = jnp.exp(jax.random.uniform(jax.random.fold_in(own, dim), (parts,), jnp.float32, low / len(split), top_value / len(split)))
        gain = gain * jnp.repeat(draws, dims[dim] // parts).reshape([-1 if axis == dim else 1 for axis in range(len(dims))])
    return gain


def shared_out(own_key, own, number, rows, amount, top, bound, skew):
    order = jax.random.permutation(own_key, amount)
    heavy_load, ordinary = shares(amount, rows * top, bound, skew, True), shares(amount, rows * top, bound, skew, False)
    places = jnp.arange(amount)

    def named(lengths, rotation):
        used = int((lengths > 0).sum())
        fixed = max(1, used // 4)
        shifted = fixed + (places - fixed + rotation * (used - fixed)) % max(1, amount - fixed)
        return jnp.zeros((amount,), jnp.int32).at[order[jnp.where(places < fixed, places, shifted)]].set(jnp.asarray(lengths, jnp.int32))

    lengths = jnp.where(number % 4 == 0, named(heavy_load, number // 4), named(ordinary, number - number // 4 - 1))
    mixed = jax.random.permutation(jax.random.fold_in(own, 3), amount)
    giver, receiver = mixed[0:amount // 2 * 2:2], mixed[1:amount // 2 * 2:2]
    margin = jnp.minimum(lengths[giver] - 1, bound - lengths[receiver]) // 2
    margin = jnp.where((giver == order[0]) | (receiver == order[0]) | (lengths[receiver] == 0), 0, jnp.maximum(margin, 0))
    shifted = jax.random.randint(jax.random.fold_in(own, 4), (amount // 2,), 0, 1 << 20) % (margin + 1)
    lengths = lengths.at[giver].add(-shifted).at[receiver].add(shifted)
    items = jnp.searchsorted(jnp.cumsum(lengths), jnp.arange(rows * top), side="right").astype(jnp.int32)
    grid = items.reshape(top, rows).T
    grid = grid[jax.random.permutation(jax.random.fold_in(own, 1), rows)]
    rotation = jax.random.randint(jax.random.fold_in(own, 2), (rows, 1), 0, top)
    return jnp.take_along_axis(grid, (jnp.arange(top)[None, :] + rotation) % top, axis=1)


def shares(count, total, bound, slope, full):
    loads = [(1 << 20) // math.isqrt(standing ** slope) + 1 for standing in range(1, count + 1)]
    largest = bound if full else min(bound, max(-(-total // count), total * loads[0] // sum(loads)))
    least = 1 if total - largest >= count - 1 else 0
    holding, surplus = [largest] + [least] * (count - 1), total - largest - least * (count - 1)
    while surplus > 0:
        movable = [i for i in range(1, count) if holding[i] < largest] or [i for i in range(1, count) if holding[i] < bound]
        mass, left = sum([loads[i] for i in movable]), surplus
        for i in movable:
            more = min(bound - holding[i], max(1, left * loads[i] // mass), surplus)
            holding[i] = holding[i] + more
            surplus = surplus - more
    return np.array(holding)


def normal_values(rng, shape, deviation, bound, cuts=(), kind=jnp.bfloat16):
    entries = jax.random.normal(rng, shape, jnp.float32) * deviation
    if len(cuts) > 0:
        entries = block_levels(rng, shape, cuts, -0.22, 0.18) * entries
    return jnp.clip(entries, min=-bound, max=bound).astype(kind)


def setup_inputs(seed: int = 0) -> dict:
    arg_keys = jax.random.split(jax.random.key(seed), 7)
    tokens = normal_values(arg_keys[0], (TOKENS, D), 1.0, 6.0, ((0, 128),))
    expert_ids_keys = jax.random.split(jax.random.fold_in(arg_keys[1], 1), TOKENS // TOK_DEV)
    expert_ids_turns = jax.random.permutation(jax.random.fold_in(arg_keys[1], 3), TOKENS // TOK_DEV)
    expert_ids = jax.vmap(lambda own, number: shared_out(jax.random.fold_in(arg_keys[1], 2), own, number, TOK_DEV, EXPERTS, TOP, CAP, 2))(expert_ids_keys, expert_ids_turns).reshape((TOKENS, TOP))
    route_gates = jnp.clip(0.049804688 + 0.54785156 * jax.random.uniform(arg_keys[2], (TOKENS, TOP), jnp.float32) ** block_levels(arg_keys[2], (TOKENS, TOP), ((0, 128),), -0.2, 0.2), 0.049804688, 0.59765625).astype(jnp.bfloat16)
    w_gate = normal_values(arg_keys[3], (EXPERTS, D, FF), D ** -0.5, 0.09375, ((0, 32), (2, 4)))
    w_up = normal_values(arg_keys[4], (EXPERTS, D, FF), D ** -0.5, 0.09375, ((0, 32), (2, 4)))
    w_down = normal_values(arg_keys[5], (EXPERTS, FF, D), FF ** -0.5, 0.15625, ((0, 32), (1, 4)))
    return dict(tokens=tokens, expert_ids=expert_ids, route_gates=route_gates, w_gate=w_gate, w_up=w_up, w_down=w_down)


def reference(tokens, expert_ids, route_gates, w_gate, w_up, w_down):
    block_rows = 128
    assigned = TOKENS * TOP
    flat_ids = expert_ids.reshape(-1).astype(jnp.int32)
    labels = jnp.arange(EXPERTS, dtype=jnp.int32)
    onehot = (flat_ids[:, None] == labels[None, :]).astype(jnp.int32)
    counts = jnp.sum(onehot, axis=0)
    ranking = jnp.sum((jnp.cumsum(onehot, axis=0) - onehot) * onehot, axis=1)
    padded = (counts + block_rows - 1) // block_rows * block_rows
    offsets = jnp.cumsum(padded) - padded
    position = jnp.sum(onehot * offsets[None, :], axis=1) + ranking
    block_count = (assigned + block_rows - 1) // block_rows + EXPERTS
    row_table = jnp.full((block_count * block_rows,), assigned, jnp.int32)
    row_table = row_table.at[position].set(jnp.arange(assigned, dtype=jnp.int32))
    starts = jnp.arange(block_count, dtype=jnp.int32) * block_rows
    owners = jnp.sum((offsets[None, :] <= starts[:, None]).astype(jnp.int32), axis=1) - 1
    owners = jnp.clip(owners, 0, EXPERTS - 1).astype(jnp.int32)
    flat_gates = jnp.concatenate([route_gates.reshape(-1).astype(jnp.float32), jnp.zeros((1,), jnp.float32)])
    token_of = jnp.concatenate([jnp.arange(assigned, dtype=jnp.int32) // TOP, jnp.full((1,), TOKENS, jnp.int32)])
    padded_tokens = jnp.concatenate([tokens, jnp.zeros((1, D), tokens.dtype)], axis=0)

    def add_block(totals, block_id):
        row_block = lax.dynamic_slice_in_dim(row_table, block_id * block_rows, block_rows)
        expert = owners[block_id]
        inputs = padded_tokens[token_of[row_block]]
        gate_acts = jnp.dot(inputs, w_gate[expert], preferred_element_type=jnp.float32)
        up_acts = jnp.dot(inputs, w_up[expert], preferred_element_type=jnp.float32)
        hidden = (jax.nn.silu(gate_acts) * up_acts).astype(jnp.bfloat16)
        sliced = hidden.reshape(block_rows, N_ATTN, SLICE).astype(jnp.float32)
        down_cut = w_down[expert].reshape(N_ATTN, SLICE, D).astype(jnp.float32)
        pieces = jnp.einsum("bsf,sfd->bsd", sliced, down_cut, precision=lax.Precision.HIGHEST).astype(jnp.bfloat16)
        routed = jnp.sum(pieces.astype(jnp.float32), axis=1)
        weighted = routed * flat_gates[row_block][:, None]
        totals = totals.at[token_of[row_block]].add(weighted, mode="drop")
        return totals, None

    totals, _ = lax.scan(add_block, jnp.zeros((TOKENS, D), jnp.float32), jnp.arange(block_count, dtype=jnp.int32))
    return totals.astype(jnp.bfloat16)
```

```python
import jax
import jax.numpy as jnp
from jax import lax
from jax.sharding import PartitionSpec as P

ORDER = ((2, 1, 0), (1, 0, 2))
AXES = ("attn", "expert")


def pairs(phase, step):
    moves = []
    for z in range(4):
        for y in range(4):
            for x in range(4):
                for core in range(2):
                    there = [z, y, x]
                    dim = ORDER[core][phase]
                    there[dim] = (there[dim] + step) % 4
                    source = ((z * 4 + y) * 4 + x) * 2 + core
                    target = ((there[0] * 4 + there[1]) * 4 + there[2]) * 2 + core
                    moves.append((source, target))
    return moves


def move(value, phase, step):
    return lax.ppermute(value, AXES, pairs(phase, step))


def swap(value):
    return lax.ppermute(value, "expert", [(i, i ^ 1) for i in range(32)])


def added(*terms):
    total = terms[0].astype(jnp.float32)
    for term in terms[1:]:
        total = total + term.astype(jnp.float32)
    return total.astype(jnp.bfloat16)


def gathered(block):
    for phase in (0, 1):
        parts = [move(block, phase, -step) for step in (1, 2, 3)]
        block = jnp.concatenate([block] + parts, axis=0)
    half = block.shape[0] // 2
    ahead = move(block, 2, -1)
    behind = move(block, 2, 1)
    low = move(ahead[:half], 2, -1)
    high = move(behind[half:], 2, 1)
    mine = [block, ahead, low, high, behind]
    return mine, [swap(part) for part in mine]


def scattered(mine, other):
    block, ahead, low, high, behind = [
        added(part, swap(sent)) for part, sent in zip(mine, other)
    ]
    half = block.shape[0] // 2
    low = move(low, 2, 1)
    high = move(high, 2, -1)
    ahead = jnp.concatenate([added(ahead[:half], low), ahead[half:]], axis=0)
    behind = jnp.concatenate([behind[:half], added(behind[half:], high)], axis=0)
    block = added(block, move(ahead, 2, 1), move(behind, 2, -1))
    for phase in (1, 0):
        rows = block.shape[0] // 4
        parts = [move(block[step * rows : (step + 1) * rows], phase, step) for step in (1, 2, 3)]
        block = added(block[:rows], *parts)
    return block


def split_rows(value, counts):
    parts, start = [], 0
    for count in counts:
        parts.append(value[start : start + count])
        start += count
    return parts


def per_device(tokens, expert_ids, route_gates, w_gate, w_up, w_down):
    rows, width = tokens.shape
    local = w_gate.shape[0]
    picks = expert_ids.shape[1]
    spare = jnp.zeros((rows, 128 - 2 * picks), tokens.dtype)
    block = jnp.concatenate([tokens, expert_ids.astype(tokens.dtype), route_gates, spare], axis=1)
    mine, other = gathered(block)
    counts = [part.shape[0] for part in mine]
    everything = jnp.concatenate(mine + other, axis=0)
    inputs = everything[:, :width]
    ids = everything[:, width : width + picks].astype(jnp.int32)
    gates = everything[:, width + picks : width + 2 * picks].astype(jnp.float32)
    owned = lax.axis_index("expert") * local + jnp.arange(local, dtype=jnp.int32)
    weight = jnp.sum(
        jnp.where(ids[None] == owned[:, None, None], gates[None], 0.0), axis=2
    )
    gate_acts = jnp.einsum("td,jdf->jtf", inputs, w_gate, preferred_element_type=jnp.float32)
    up_acts = jnp.einsum("td,jdf->jtf", inputs, w_up, preferred_element_type=jnp.float32)
    hidden = (jax.nn.silu(gate_acts) * up_acts * weight[:, :, None]).astype(jnp.bfloat16)
    partial = jnp.einsum("jtf,jfd->td", hidden, w_down, preferred_element_type=jnp.float32)
    parts = split_rows(partial.astype(jnp.bfloat16), counts + counts)
    return scattered(parts[: len(counts)], parts[len(counts) :])


def solution(mesh):
    placed = (
        P(("attn", "expert"), None),
        P(("attn", "expert"), None),
        P(("attn", "expert"), None),
        P("expert", None, "attn"),
        P("expert", None, "attn"),
        P("expert", "attn", None),
    )
    return jax.shard_map(
        per_device,
        mesh=mesh,
        in_specs=placed,
        out_specs=P(("attn", "expert"), None),
        check_vma=False,
    )
```

```python
import functools

import jax
import jax.numpy as jnp
from jax import lax
from jax.experimental import pallas as pl
from jax.experimental.pallas import tpu as pltpu
from jax.sharding import PartitionSpec as P

LONG = (0, 2)
AXES = ("attn", "expert")
NODES = [(z, y, x, core) for z in range(4) for y in range(4) for x in range(4) for core in range(2)]


def place(node):
    z, y, x, core = node
    return ((z * 4 + y) * 4 + x) * 2 + core


def pairs(step):
    moves = []
    for node in NODES:
        there = list(node)
        dim = LONG[node[3]]
        there[dim] = (there[dim] + step) % 4
        moves.append((place(node), place(there)))
    return moves


def planes():
    groups = {}
    for node in NODES:
        groups.setdefault((node[3], node[LONG[node[3]]]), []).append(place(node))
    return [groups[key] for key in sorted(groups)]


def move(value, step):
    return lax.ppermute(value, AXES, pairs(step))


def swap(value):
    return lax.ppermute(value, AXES, [(i, i ^ 1) for i in range(128)])


def in_plane(value):
    return lax.all_to_all(value, AXES, 0, 0, axis_index_groups=planes(), tiled=True)


def added(*terms):
    total = terms[0].astype(jnp.float32)
    for term in terms[1:]:
        total = total + term.astype(jnp.float32)
    return total.astype(jnp.bfloat16)


def expert_kernel(counts, local, width, hidden, loads, *refs):
    pieces = refs[: len(counts)]
    weights = refs[len(counts) : len(counts) + 3]
    own_ref, other_ref = refs[len(counts) + 3 : len(counts) + 5]
    scratch = refs[len(counts) + 5 :]
    copies = []
    if loads:
        held, (rows_ref, hidden_ref, sems) = scratch[:3], scratch[3:]
        for j in range(local):
            for kind in range(3):
                at = pl.ds(j * hidden, hidden) if kind == 2 else j
                copies.append(
                    pltpu.make_async_copy(
                        weights[kind].at[at], held[kind].at[at], sems.at[3 * j + kind]
                    )
                )
        for copy in (0, 1, 3, 4, 2, 5):
            copies[copy].start()
        weights = held
    else:
        rows_ref, hidden_ref = scratch
    gate_ref, up_ref, down_ref = weights
    start = 0
    for count, piece in zip(counts, pieces):
        rows_ref[start : start + count, :] = piece[...]
        start += count
    routing = rows_ref[:, width:].astype(jnp.float32)
    lane = lax.broadcasted_iota(jnp.int32, routing.shape, 1)
    first = (lax.axis_index("expert") * local).astype(jnp.float32)
    for j in range(local):
        hit = jnp.where((routing == first + j) & (lane < 8), 1.0, 0.0)
        weight = jnp.sum(pltpu.roll(hit, 8, 1) * routing, axis=1, keepdims=True)
        if loads:
            copies[3 * j].wait()
            copies[3 * j + 1].wait()
        inputs = rows_ref[:, :width]
        acts = []
        for part in range(3):
            if part == 0:
                columns = gate_ref[j, :, 0:256]
            elif part == 1:
                columns = jnp.concatenate([gate_ref[j, :, 256:384], up_ref[j, :, 0:128]], axis=1)
            else:
                columns = up_ref[j, :, 128:384]
            acts.append(jnp.dot(inputs, columns, preferred_element_type=jnp.float32))
        gates = [acts[0][:, :128], acts[0][:, 128:], acts[1][:, :128]]
        ups = [acts[1][:, 128:], acts[2][:, :128], acts[2][:, 128:]]
        for s in range(3):
            value = gates[s] / (1.0 + jnp.exp(-gates[s])) * ups[s] * weight
            at = j * hidden + s * 128
            hidden_ref[:, at : at + 128] = value.astype(jnp.bfloat16)
    if loads:
        for j in range(local):
            copies[3 * j + 2].wait()
    half = own_ref.shape[0]

    def down(n, carry):
        at = pl.ds(pl.multiple_of(n * 256, 256), 256)
        result = jnp.dot(hidden_ref[...], down_ref[:, at], preferred_element_type=jnp.float32)
        result = result.astype(jnp.bfloat16)
        own_ref[:, at] = result[:half]
        other_ref[:, at] = result[half:]
        return carry

    lax.fori_loop(0, width // 256, down, 0)


def experts(pieces, w_gate, w_up, w_down, loads=False):
    counts = tuple(piece.shape[0] for piece in pieces)
    total = sum(counts)
    local, width, hidden = w_gate.shape
    vmem = pl.BlockSpec(memory_space=pltpu.VMEM)
    space = pltpu.HBM if loads else pltpu.VMEM
    weights = [pltpu.with_memory_space_constraint(v, space) for v in (w_gate, w_up, w_down)]
    held = [pltpu.with_memory_space_constraint(v, pltpu.VMEM) for v in pieces]
    outs = [pltpu.VMEM((total // 2, width), jnp.bfloat16)] * 2
    scratch = [
        pltpu.VMEM((total, pieces[0].shape[1]), jnp.bfloat16),
        pltpu.VMEM((total, local * hidden), jnp.bfloat16),
    ]
    if loads:
        outs += [pltpu.VMEM(v.shape, v.dtype) for v in weights]
        scratch.append(pltpu.SemaphoreType.DMA((3 * local,)))
    return pl.pallas_call(
        functools.partial(expert_kernel, counts, local, width, hidden, loads),
        out_shape=outs,
        in_specs=[vmem] * len(counts) + [pl.BlockSpec(memory_space=pltpu.HBM) if loads else vmem] * 3,
        out_specs=[vmem] * len(outs),
        scratch_shapes=scratch,
        compiler_params=pltpu.CompilerParams(vmem_limit_bytes=16 << 20),
        cost_estimate=pl.CostEstimate(
            flops=6 * total * local * hidden * width,
            bytes_accessed=4 * total * width,
            transcendentals=total * local * hidden,
        ),
    )(*held, *weights)


def after(value, *others):
    return lax.optimization_barrier((value, *others))[0]


def per_device(tokens, expert_ids, route_gates, w_gate, w_up, w_down):
    rows, width = tokens.shape
    picks = expert_ids.shape[1]
    local, _, hidden = w_gate.shape
    w_down = w_down.reshape(local * hidden, width)
    spare = jnp.zeros((rows, 128 - 2 * picks), tokens.dtype)
    block = jnp.concatenate([tokens, expert_ids.astype(tokens.dtype), route_gates, spare], axis=1)
    near = in_plane(jnp.broadcast_to(block[None], (16, *block.shape)))
    near = near.reshape(16 * rows, block.shape[1])
    half = 8 * rows
    near_a, near_b = near[:half], near[half:]
    ahead_a, behind_b = move(near_a, -1), move(near_b, 1)
    ahead_b, behind_a = move(near_b, -1), move(near_a, 1)

    own0, other0, *weights = experts((near, swap(near)), w_gate, w_up, w_down, True)
    ahead_a, behind_b = after(ahead_a, other0), after(behind_b, other0)
    far_a, far_b = move(ahead_a, -1), move(behind_b, 1)
    own1, other1 = experts((ahead_a, behind_b, swap(ahead_a), swap(behind_b)), *weights)
    own2, other2 = experts((ahead_b, behind_a, swap(ahead_b), swap(behind_a)), *weights)
    own3, other3 = experts((far_a, far_b, swap(far_a), swap(far_b)), *weights)

    sum1 = added(own1, swap(other1))
    got_a, got_b = move(sum1[:half], 1), move(sum1[half:], -1)
    sum3 = added(own3, swap(other3))
    through_a, through_b = move(sum3[:half], -1), move(sum3[half:], 1)
    back2 = swap(other2)
    more_b = move(added(own2[:half], back2[:half], through_b), 1)
    more_a = move(added(own2[half:], back2[half:], through_a), -1)
    back0 = swap(other0)
    total = jnp.concatenate(
        [
            added(own0[:half], back0[:half], got_a, more_a),
            added(own0[half:], back0[half:], got_b, more_b),
        ],
        axis=0,
    )
    returned = in_plane(total.reshape(16, rows, width))
    return jnp.sum(returned.astype(jnp.float32), axis=0).astype(jnp.bfloat16)


def solution(mesh):
    placed = (
        P(AXES, None),
        P(AXES, None),
        P(AXES, None),
        P("expert", None, "attn"),
        P("expert", None, "attn"),
        P("expert", "attn", None),
    )
    return jax.shard_map(
        per_device, mesh=mesh, in_specs=placed, out_specs=P(AXES, None), check_vma=False
    )
```

```python
import functools

import jax
import jax.numpy as jnp
from jax import lax
from jax.experimental import pallas as pl
from jax.experimental.pallas import tpu as pltpu
from jax.sharding import PartitionSpec as P


LONG = (0, 2)
AXES = ("attn", "expert")
NODES = [(z, y, x, core) for z in range(4) for y in range(4) for x in range(4) for core in range(2)]


def place(node):
    z, y, x, core = node
    return ((z * 4 + y) * 4 + x) * 2 + core


def pairs(step):
    moves = []
    for node in NODES:
        there = list(node)
        dim = LONG[node[3]]
        there[dim] = (there[dim] + step) % 4
        moves.append((place(node), place(there)))
    return moves


def planes():
    groups = {}
    for node in NODES:
        groups.setdefault((node[3], node[LONG[node[3]]]), []).append(place(node))
    return [groups[key] for key in sorted(groups)]


def move(value, step):
    return lax.ppermute(value, AXES, pairs(step))


def swap(value):
    return lax.ppermute(value, AXES, [(i, i ^ 1) for i in range(128)])


def in_plane(value):
    return lax.all_to_all(value, AXES, 0, 0, axis_index_groups=planes(), tiled=True)


def added(*terms):
    total = terms[0].astype(jnp.float32)
    for term in terms[1:]:
        total = total + term.astype(jnp.float32)
    return total.astype(jnp.bfloat16)


def expert_kernel(counts, local, width, hidden, loads, *refs):
    pieces = refs[: len(counts)]
    weights = refs[len(counts) : len(counts) + 3]
    own_ref, other_ref = refs[len(counts) + 3 : len(counts) + 5]
    scratch = refs[len(counts) + 5 :]
    copies = []
    if loads:
        held, (rows_ref, hidden_ref, sems) = scratch[:3], scratch[3:]
        for j in range(local):
            for kind in range(3):
                at = pl.ds(j * hidden, hidden) if kind == 2 else j
                copies.append(
                    pltpu.make_async_copy(
                        weights[kind].at[at], held[kind].at[at], sems.at[3 * j + kind]
                    )
                )
        for copy in (0, 1, 3, 4, 2, 5):
            copies[copy].start()
        weights = held
    else:
        rows_ref, hidden_ref = scratch
    gate_ref, up_ref, down_ref = weights
    start = 0
    for count, piece in zip(counts, pieces):
        rows_ref[start : start + count, :] = piece[...]
        start += count
    routing = rows_ref[:, width:].astype(jnp.float32)
    lane = lax.broadcasted_iota(jnp.int32, routing.shape, 1)
    first = (lax.axis_index("expert") * local).astype(jnp.float32)
    for j in range(local):
        hit = jnp.where((routing == first + j) & (lane < 8), 1.0, 0.0)
        weight = jnp.sum(pltpu.roll(hit, 8, 1) * routing, axis=1, keepdims=True)
        if loads:
            copies[3 * j].wait()
            copies[3 * j + 1].wait()
        inputs = rows_ref[:, :width]
        acts = []
        for part in range(3):
            if part == 0:
                columns = gate_ref[j, :, 0:256]
            elif part == 1:
                columns = jnp.concatenate([gate_ref[j, :, 256:384], up_ref[j, :, 0:128]], axis=1)
            else:
                columns = up_ref[j, :, 128:384]
            acts.append(jnp.dot(inputs, columns, preferred_element_type=jnp.float32))
        gates = [acts[0][:, :128], acts[0][:, 128:], acts[1][:, :128]]
        ups = [acts[1][:, 128:], acts[2][:, :128], acts[2][:, 128:]]
        for s in range(3):
            value = gates[s] / (1.0 + jnp.exp(-gates[s])) * ups[s] * weight
            at = j * hidden + s * 128
            hidden_ref[:, at : at + 128] = value.astype(jnp.bfloat16)
    if loads:
        for j in range(local):
            copies[3 * j + 2].wait()
    half = own_ref.shape[0]

    result = jnp.dot(hidden_ref[...], down_ref[...], preferred_element_type=jnp.float32)
    result = result.astype(jnp.bfloat16)
    own_ref[...] = result[:half]
    other_ref[...] = result[half:]


def experts(pieces, w_gate, w_up, w_down, loads=False):
    counts = tuple(piece.shape[0] for piece in pieces)
    total = sum(counts)
    local, width, hidden = w_gate.shape
    vmem = pl.BlockSpec(memory_space=pltpu.VMEM)
    space = pltpu.HBM if loads else pltpu.VMEM
    weights = [pltpu.with_memory_space_constraint(v, space) for v in (w_gate, w_up, w_down)]
    held = [pltpu.with_memory_space_constraint(v, pltpu.VMEM) for v in pieces]
    outs = [pltpu.VMEM((total // 2, width), jnp.bfloat16)] * 2
    scratch = [
        pltpu.VMEM((total, pieces[0].shape[1]), jnp.bfloat16),
        pltpu.VMEM((total, local * hidden), jnp.bfloat16),
    ]
    if loads:
        outs += [pltpu.VMEM(v.shape, v.dtype) for v in weights]
        scratch.append(pltpu.SemaphoreType.DMA((3 * local,)))
    return pl.pallas_call(
        functools.partial(expert_kernel, counts, local, width, hidden, loads),
        out_shape=outs,
        in_specs=[vmem] * len(counts) + [pl.BlockSpec(memory_space=pltpu.HBM) if loads else vmem] * 3,
        out_specs=[vmem] * len(outs),
        scratch_shapes=scratch,
        compiler_params=pltpu.CompilerParams(vmem_limit_bytes=16 << 20),
        cost_estimate=pl.CostEstimate(
            flops=6 * total * local * hidden * width,
            bytes_accessed=4 * total * width,
            transcendentals=total * local * hidden,
        ),
    )(*held, *weights)


def after(values, *others):
    return lax.optimization_barrier((*values, *others))[: len(values)]


def per_device(tokens, expert_ids, route_gates, w_gate, w_up, w_down):
    rows, width = tokens.shape
    picks = expert_ids.shape[1]
    local, _, hidden = w_gate.shape
    w_down = w_down.reshape(local * hidden, width)
    spare = jnp.zeros((rows, 128 - 2 * picks), tokens.dtype)
    block = jnp.concatenate([tokens, expert_ids.astype(tokens.dtype), route_gates, spare], axis=1)
    near = in_plane(jnp.broadcast_to(block[None], (16, *block.shape)))
    near = near.reshape(16 * rows, block.shape[1])
    half = 8 * rows
    near_a, near_b = near[:half], near[half:]
    ahead_a = move(near_a, -1)
    behind_b = move(near_b, 1)

    own0, other0, *weights = experts((near, swap(near)), w_gate, w_up, w_down, True)
    ahead_a, behind_b, near_a, near_b = after((ahead_a, behind_b, near_a, near_b), other0)
    far_a = move(ahead_a, -1)
    far_b = move(behind_b, 1)
    ahead_b = move(near_b, -1)
    behind_a = move(near_a, 1)
    pieces = (ahead_a, behind_b, swap(ahead_a), swap(behind_b))
    own1, other1 = experts(pieces, *weights)
    sum1 = added(own1, swap(other1))

    far_a, far_b = after((far_a, far_b), other1)
    pieces = (far_a, far_b, swap(far_a), swap(far_b))
    own2, other2 = experts(pieces, *weights)
    sum2 = added(own2, swap(other2))
    through_a = move(sum2[:half], -1)
    through_b = move(sum2[half:], 1)
    got_a = move(sum1[:half], 1)
    got_b = move(sum1[half:], -1)

    ahead_b, behind_a = after((ahead_b, behind_a), other2)
    pieces = (ahead_b, behind_a, swap(ahead_b), swap(behind_a))
    own3, other3 = experts(pieces, *weights)
    sum3 = added(own3, swap(other3))
    more_b = move(added(sum3[:half], through_b), 1)
    more_a = move(added(sum3[half:], through_a), -1)
    sum0 = added(own0, swap(other0))
    total = jnp.concatenate(
        [added(sum0[:half], got_a, more_a), added(sum0[half:], got_b, more_b)], axis=0
    )
    returned = in_plane(total.reshape(16, rows, width))
    return jnp.sum(returned.astype(jnp.float32), axis=0).astype(jnp.bfloat16)


def solution(mesh):
    placed = (
        P(AXES, None),
        P(AXES, None),
        P(AXES, None),
        P("expert", None, "attn"),
        P("expert", None, "attn"),
        P("expert", "attn", None),
    )

    return jax.shard_map(
        per_device, mesh=mesh, in_specs=placed, out_specs=P(AXES, None), check_vma=False
    )
```

```python
import functools

import jax
import jax.numpy as jnp
from jax import lax
from jax.experimental import pallas as pl
from jax.experimental.pallas import tpu as pltpu
from jax.sharding import PartitionSpec as P


DIMS = ((2, 1, 0), (1, 0, 2))
AXES = ("attn", "expert")
NODES = [(z, y, x, core) for z in range(4) for y in range(4) for x in range(4) for core in range(2)]


def place(node):
    z, y, x, core = node
    return ((z * 4 + y) * 4 + x) * 2 + core


def pairs(phase, step):
    moves = []
    for node in NODES:
        there = list(node)
        dim = DIMS[node[3]][phase]
        there[dim] = (there[dim] + step) % 4
        moves.append((place(node), place(there)))
    return moves


def move(value, step, phase=2):
    return lax.ppermute(value, AXES, pairs(phase, step))


def swap(value):
    return lax.ppermute(value, AXES, [(i, i ^ 1) for i in range(128)])


def added(*terms):
    total = terms[0].astype(jnp.float32)
    for term in terms[1:]:
        total = total + term.astype(jnp.float32)
    return total.astype(jnp.bfloat16)


def load_kernel(count, *refs):
    sources, targets, sems = refs[:count], refs[count : 2 * count], refs[2 * count]
    copies = [pltpu.make_async_copy(sources[i], targets[i], sems.at[i]) for i in range(count)]
    for copy in copies:
        copy.start()
    for copy in copies:
        copy.wait()


def loaded(*weights):
    count = len(weights)
    return pl.pallas_call(
        functools.partial(load_kernel, count),
        out_shape=[pltpu.VMEM(v.shape, v.dtype) for v in weights],
        in_specs=[pl.BlockSpec(memory_space=pltpu.HBM)] * count,
        out_specs=[pl.BlockSpec(memory_space=pltpu.VMEM)] * count,
        scratch_shapes=[pltpu.SemaphoreType.DMA((count,))],
        compiler_params=pltpu.CompilerParams(vmem_limit_bytes=1 << 20),
        cost_estimate=pl.CostEstimate(flops=0, bytes_accessed=16_000_000, transcendentals=0),
    )(*[pltpu.with_memory_space_constraint(v, pltpu.HBM) for v in weights])


def expert_kernel(counts, local, width, hidden, *refs):
    pieces = refs[: len(counts)]
    gate_ref, up_ref, down_ref = refs[len(counts) : len(counts) + 3]
    own_ref, other_ref, rows_ref, hidden_ref = refs[len(counts) + 3 :]
    start = 0
    for count, piece in zip(counts, pieces):
        rows_ref[start : start + count, :] = piece[...]
        start += count
    routing = rows_ref[:, width:].astype(jnp.float32)
    lane = lax.broadcasted_iota(jnp.int32, routing.shape, 1)
    first = (lax.axis_index("expert") * local).astype(jnp.float32)
    for j in range(local):
        hit = jnp.where((routing == first + j) & (lane < 8), 1.0, 0.0)
        weight = jnp.sum(pltpu.roll(hit, 8, 1) * routing, axis=1, keepdims=True)
        inputs = rows_ref[:, :width]
        acts = []
        for part in range(3):
            if part == 0:
                columns = gate_ref[j, :, 0:256]
            elif part == 1:
                columns = jnp.concatenate([gate_ref[j, :, 256:384], up_ref[j, :, 0:128]], axis=1)
            else:
                columns = up_ref[j, :, 128:384]
            acts.append(jnp.dot(inputs, columns, preferred_element_type=jnp.float32))
        gates = [acts[0][:, :128], acts[0][:, 128:], acts[1][:, :128]]
        ups = [acts[1][:, 128:], acts[2][:, :128], acts[2][:, 128:]]
        for s in range(3):
            value = gates[s] / (1.0 + jnp.exp(-gates[s])) * ups[s] * weight
            at = j * hidden + s * 128
            hidden_ref[:, at : at + 128] = value.astype(jnp.bfloat16)
    half = own_ref.shape[0]

    result = jnp.dot(hidden_ref[...], down_ref[...], preferred_element_type=jnp.float32)
    result = result.astype(jnp.bfloat16)
    own_ref[...] = result[:half]
    other_ref[...] = result[half:]


def experts(pieces, w_gate, w_up, w_down):
    counts = tuple(piece.shape[0] for piece in pieces)
    total = sum(counts)
    local, width, hidden = w_gate.shape
    vmem = pl.BlockSpec(memory_space=pltpu.VMEM)
    held = [pltpu.with_memory_space_constraint(v, pltpu.VMEM) for v in (*pieces, w_gate, w_up, w_down)]
    return pl.pallas_call(
        functools.partial(expert_kernel, counts, local, width, hidden),
        out_shape=[pltpu.VMEM((total // 2, width), jnp.bfloat16)] * 2,
        in_specs=[vmem] * len(held),
        out_specs=[vmem] * 2,
        scratch_shapes=[
            pltpu.VMEM((total, pieces[0].shape[1]), jnp.bfloat16),
            pltpu.VMEM((total, local * hidden), jnp.bfloat16),
        ],
        compiler_params=pltpu.CompilerParams(vmem_limit_bytes=16 << 20),
        cost_estimate=pl.CostEstimate(
            flops=6 * total * local * hidden * width,
            bytes_accessed=4 * total * width,
            transcendentals=total * local * hidden,
        ),
    )(*held)


def after(values, *others):
    return lax.optimization_barrier((*values, *others))[: len(values)]


def per_device(tokens, expert_ids, route_gates, w_gate, w_up, w_down):
    rows, width = tokens.shape
    picks = expert_ids.shape[1]
    local, _, hidden = w_gate.shape
    half = 8 * rows
    spare = jnp.zeros((rows, 128 - 2 * picks), tokens.dtype)
    block = jnp.concatenate([tokens, expert_ids.astype(tokens.dtype), route_gates, spare], axis=1)
    (gate,) = loaded(w_gate)
    one = [move(block, -step, 0) for step in (1, 2, 3)]
    up, down = loaded(w_up, w_down.reshape(local * hidden, width))
    weights = (gate, up, down)
    block = jnp.concatenate([block] + one, axis=0)
    two = [move(block, -step, 1) for step in (1, 2, 3)]
    near_a = jnp.concatenate([block, two[0]], axis=0)
    near_b = jnp.concatenate([two[1], two[2]], axis=0)
    ahead_a = move(near_a, -1)
    behind_b = move(near_b, 1)

    own0, other0 = experts((near_a, near_b, swap(near_a), swap(near_b)), *weights)
    ahead_a, behind_b, near_a, near_b = after((ahead_a, behind_b, near_a, near_b), other0)
    far_a = move(ahead_a, -1)
    far_b = move(behind_b, 1)
    ahead_b = move(near_b, -1)
    behind_a = move(near_a, 1)
    pieces = (ahead_a, behind_b, swap(ahead_a), swap(behind_b))
    own1, other1 = experts(pieces, *weights)
    sum1 = added(own1, swap(other1))

    far_a, far_b = after((far_a, far_b), other1)
    pieces = (far_a, far_b, swap(far_a), swap(far_b))
    own2, other2 = experts(pieces, *weights)
    sum2 = added(own2, swap(other2))
    through_a = move(sum2[:half], -1)
    through_b = move(sum2[half:], 1)
    got_a = move(sum1[:half], 1)
    got_b = move(sum1[half:], -1)

    ahead_b, behind_a = after((ahead_b, behind_a), other2)
    pieces = (ahead_b, behind_a, swap(ahead_b), swap(behind_a))
    own3, other3 = experts(pieces, *weights)
    sum3 = added(own3, swap(other3))
    more_b = move(added(sum3[:half], through_b), 1)
    more_a = move(added(sum3[half:], through_a), -1)
    sum0 = added(own0, swap(other0))
    quarter = half // 2
    parts = []
    for side, got, more in ((sum0[:half], got_a, more_a), (sum0[half:], got_b, more_b)):
        for at in (0, quarter):
            parts.append(added(*[v[at : at + quarter] for v in (side, got, more)]))
    for phase in (1, 0):
        arrived = [move(parts[step], step, phase) for step in (1, 2, 3)]
        block = added(parts[0], *arrived)
        parts = [block[step * rows : (step + 1) * rows] for step in range(4)]
    return block


def solution(mesh):
    placed = (
        P(AXES, None),
        P(AXES, None),
        P(AXES, None),
        P("expert", None, "attn"),
        P("expert", None, "attn"),
        P("expert", "attn", None),
    )

    return jax.shard_map(
        per_device, mesh=mesh, in_specs=placed, out_specs=P(AXES, None), check_vma=False
    )
```

```python
import functools

import jax
import jax.numpy as jnp
from jax import lax
from jax.experimental import pallas as pl
from jax.experimental.pallas import tpu as pltpu
from jax.sharding import PartitionSpec as P


DIMS = ((2, 1, 0), (1, 0, 2))
AXES = ("attn", "expert")
NODES = [(z, y, x, core) for z in range(4) for y in range(4) for x in range(4) for core in range(2)]


def place(node):
    z, y, x, core = node
    return ((z * 4 + y) * 4 + x) * 2 + core


def pairs(phase, step):
    moves = []
    for node in NODES:
        there = list(node)
        dim = DIMS[node[3]][phase]
        there[dim] = (there[dim] + step) % 4
        moves.append((place(node), place(there)))
    return moves


def move(value, step, phase=2):
    return lax.ppermute(value, AXES, pairs(phase, step))


def swap(value):
    return lax.ppermute(value, AXES, [(i, i ^ 1) for i in range(128)])


def added(*terms):
    total = terms[0].astype(jnp.float32)
    for term in terms[1:]:
        total = total + term.astype(jnp.float32)
    return total.astype(jnp.bfloat16)


def load_kernel(count, *refs):
    sources, targets, sems = refs[:count], refs[count : 2 * count], refs[2 * count]
    copies = [pltpu.make_async_copy(sources[i], targets[i], sems.at[i]) for i in range(count)]
    for copy in copies:
        copy.start()
    for copy in copies:
        copy.wait()


def loaded(*weights):
    count = len(weights)
    return pl.pallas_call(
        functools.partial(load_kernel, count),
        out_shape=[pltpu.VMEM(v.shape, v.dtype) for v in weights],
        in_specs=[pl.BlockSpec(memory_space=pltpu.HBM)] * count,
        out_specs=[pl.BlockSpec(memory_space=pltpu.VMEM)] * count,
        scratch_shapes=[pltpu.SemaphoreType.DMA((count,))],
        compiler_params=pltpu.CompilerParams(vmem_limit_bytes=1 << 20),
        cost_estimate=pl.CostEstimate(flops=0, bytes_accessed=16_000_000, transcendentals=0),
    )(*[pltpu.with_memory_space_constraint(v, pltpu.HBM) for v in weights])


def expert_kernel(counts, local, width, hidden, *refs):
    pieces = refs[: len(counts)]
    gate_ref, up_ref, down_ref = refs[len(counts) : len(counts) + 3]
    own_ref, other_ref, rows_ref, hidden_ref = refs[len(counts) + 3 :]
    start = 0
    for count, piece in zip(counts, pieces):
        rows_ref[start : start + count, :] = piece[...]
        start += count
    routing = rows_ref[:, width:].astype(jnp.float32)
    lane = lax.broadcasted_iota(jnp.int32, routing.shape, 1)
    first = (lax.axis_index("expert") * local).astype(jnp.float32)
    for j in range(local):
        hit = jnp.where((routing == first + j) & (lane < 8), 1.0, 0.0)
        weight = jnp.sum(pltpu.roll(hit, 8, 1) * routing, axis=1, keepdims=True)
        inputs = rows_ref[:, :width]
        acts = []
        for part in range(3):
            if part == 0:
                columns = gate_ref[j, :, 0:256]
            elif part == 1:
                columns = jnp.concatenate([gate_ref[j, :, 256:384], up_ref[j, :, 0:128]], axis=1)
            else:
                columns = up_ref[j, :, 128:384]
            acts.append(jnp.dot(inputs, columns, preferred_element_type=jnp.float32))
        gates = [acts[0][:, :128], acts[0][:, 128:], acts[1][:, :128]]
        ups = [acts[1][:, 128:], acts[2][:, :128], acts[2][:, 128:]]
        for s in range(3):
            value = gates[s] / (1.0 + jnp.exp(-gates[s])) * ups[s] * weight
            at = j * hidden + s * 128
            hidden_ref[:, at : at + 128] = value.astype(jnp.bfloat16)
    half = own_ref.shape[0]

    result = jnp.dot(hidden_ref[...], down_ref[...], preferred_element_type=jnp.float32)
    result = result.astype(jnp.bfloat16)
    own_ref[...] = result[:half]
    other_ref[...] = result[half:]


def experts(pieces, w_gate, w_up, w_down):
    counts = tuple(piece.shape[0] for piece in pieces)
    total = sum(counts)
    local, width, hidden = w_gate.shape
    vmem = pl.BlockSpec(memory_space=pltpu.VMEM)
    held = [pltpu.with_memory_space_constraint(v, pltpu.VMEM) for v in (*pieces, w_gate, w_up, w_down)]
    return pl.pallas_call(
        functools.partial(expert_kernel, counts, local, width, hidden),
        out_shape=[pltpu.VMEM((total // 2, width), jnp.bfloat16)] * 2,
        in_specs=[vmem] * len(held),
        out_specs=[vmem] * 2,
        scratch_shapes=[
            pltpu.VMEM((total, pieces[0].shape[1]), jnp.bfloat16),
            pltpu.VMEM((total, local * hidden), jnp.bfloat16),
        ],
        compiler_params=pltpu.CompilerParams(vmem_limit_bytes=16 << 20),
        cost_estimate=pl.CostEstimate(
            flops=6 * total * local * hidden * width,
            bytes_accessed=4 * total * width,
            transcendentals=total * local * hidden,
        ),
    )(*held)


def after(values, *others):
    return lax.optimization_barrier((*values, *others))[: len(values)]


def per_device(tokens, expert_ids, route_gates, w_gate, w_up, w_down):
    rows, width = tokens.shape
    picks = expert_ids.shape[1]
    local, _, hidden = w_gate.shape
    half = 8 * rows
    spare = jnp.zeros((rows, 128 - 2 * picks), tokens.dtype)
    block = jnp.concatenate([tokens, expert_ids.astype(tokens.dtype), route_gates, spare], axis=1)
    (gate,) = loaded(w_gate)
    one = [move(block, -step, 0) for step in (1, 2, 3)]
    up, down = loaded(w_up, w_down.reshape(local * hidden, width))
    weights = (gate, up, down)
    block = jnp.concatenate([block] + one, axis=0)
    two = [move(block, -step, 1) for step in (1, 2, 3)]
    near_a = jnp.concatenate([block, two[0]], axis=0)
    near_b = jnp.concatenate([two[1], two[2]], axis=0)
    ahead_a = move(near_a, -1)
    behind_b = move(near_b, 1)

    own0, other0 = experts((near_a, near_b, swap(near_a), swap(near_b)), *weights)
    ahead_a, behind_b = after((ahead_a, behind_b), other0)
    far_a = move(ahead_a, -1)
    far_b = move(behind_b, 1)
    ahead_b = move(near_b, -1)
    behind_a = move(near_a, 1)
    pieces = (ahead_a, behind_b, swap(ahead_a), swap(behind_b))
    own1, other1 = experts(pieces, *weights)
    back1 = swap(other1)

    far_a, far_b = after((far_a, far_b), other1)
    pieces = (far_a, far_b, swap(far_a), swap(far_b))
    own2, other2 = experts(pieces, *weights)
    back2 = swap(other2)
    through_a = move(added(own2[:half], back2[:half]), -1)
    through_b = move(added(own2[half:], back2[half:]), 1)
    got_a = move(added(own1[:half], back1[:half]), 1)
    got_b = move(added(own1[half:], back1[half:]), -1)

    ahead_b, behind_a = after((ahead_b, behind_a), other2)
    pieces = (ahead_b, behind_a, swap(ahead_b), swap(behind_a))
    own3, other3 = experts(pieces, *weights)
    sum3 = added(own3, swap(other3))
    more_b = move(added(sum3[:half], through_b), 1)
    more_a = move(added(sum3[half:], through_a), -1)
    sum0 = added(own0, swap(other0))
    quarter = half // 2
    parts = []
    for side, got, more in ((sum0[:half], got_a, more_a), (sum0[half:], got_b, more_b)):
        for at in (0, quarter):
            parts.append(added(*[v[at : at + quarter] for v in (side, got, more)]))
    for phase in (1, 0):
        arrived = [move(parts[step], step, phase) for step in (1, 2, 3)]
        block = added(parts[0], *arrived)
        parts = [block[step * rows : (step + 1) * rows] for step in range(4)]
    return block


def solution(mesh):
    placed = (
        P(AXES, None),
        P(AXES, None),
        P(AXES, None),
        P("expert", None, "attn"),
        P("expert", None, "attn"),
        P("expert", "attn", None),
    )

    return jax.shard_map(
        per_device, mesh=mesh, in_specs=placed, out_specs=P(AXES, None), check_vma=False
    )
```

```python
import functools

import jax
import jax.numpy as jnp
from jax import lax
from jax.experimental import pallas as pl
from jax.experimental.pallas import tpu as pltpu
from jax.sharding import PartitionSpec as P


DIMS = ((1, 2, 0), (0, 1, 2))
AXES = ("attn", "expert")
NODES = [(z, y, x, core) for z in range(4) for y in range(4) for x in range(4) for core in range(2)]


def place(node):
    z, y, x, core = node
    return ((z * 4 + y) * 4 + x) * 2 + core


def pairs(phase, step):
    moves = []
    for node in NODES:
        there = list(node)
        dim = DIMS[node[3]][phase]
        there[dim] = (there[dim] + step) % 4
        moves.append((place(node), place(there)))
    return moves


def move(value, step, phase=2):
    return lax.ppermute(value, AXES, pairs(phase, step))


def swap(value):
    return lax.ppermute(value, AXES, [(i, i ^ 1) for i in range(128)])


def added(*terms):
    total = terms[0].astype(jnp.float32)
    for term in terms[1:]:
        total = total + term.astype(jnp.float32)
    return total.astype(jnp.bfloat16)


def load_kernel(expert, whole_ref, down_ref, held_ref, kept_ref, sems):
    copies = [
        pltpu.make_async_copy(whole_ref, held_ref, sems.at[0]),
        pltpu.make_async_copy(down_ref.at[expert], kept_ref, sems.at[1]),
    ]
    for copy in copies:
        copy.start()
    for copy in copies:
        copy.wait()


def loaded(whole, w_down, expert):
    return pl.pallas_call(
        functools.partial(load_kernel, expert),
        out_shape=[pltpu.VMEM(whole.shape, whole.dtype), pltpu.VMEM(w_down.shape[1:], w_down.dtype)],
        in_specs=[pl.BlockSpec(memory_space=pltpu.HBM)] * 2,
        out_specs=[pl.BlockSpec(memory_space=pltpu.VMEM)] * 2,
        scratch_shapes=[pltpu.SemaphoreType.DMA((2,))],
        compiler_params=pltpu.CompilerParams(vmem_limit_bytes=1 << 20),
        cost_estimate=pl.CostEstimate(flops=0, bytes_accessed=20_000_000, transcendentals=0),
    )(*[pltpu.with_memory_space_constraint(v, pltpu.HBM) for v in (whole, w_down)])


def expert_kernel(counts, local, width, hidden, *refs):
    pieces = refs[: len(counts)]
    gate_ref, up_ref, *down_refs = refs[len(counts) : len(counts) + 2 + local]
    own_ref, other_ref, rows_ref, hidden_ref = refs[len(counts) + 2 + local :]
    start = 0
    for count, piece in zip(counts, pieces):
        rows_ref[start : start + count, :] = piece[...]
        start += count
    routing = rows_ref[:, width:].astype(jnp.float32)
    lane = lax.broadcasted_iota(jnp.int32, routing.shape, 1)
    first = (lax.axis_index("expert") * local).astype(jnp.float32)
    for j in range(local):
        hit = jnp.where((routing == first + j) & (lane < 8), 1.0, 0.0)
        weight = jnp.sum(pltpu.roll(hit, 8, 1) * routing, axis=1, keepdims=True)
        inputs = rows_ref[:, :width]
        acts = []
        for part in range(3):
            if part == 0:
                columns = gate_ref[j, :, 0:256]
            elif part == 1:
                columns = jnp.concatenate([gate_ref[j, :, 256:384], up_ref[j, :, 0:128]], axis=1)
            else:
                columns = up_ref[j, :, 128:384]
            acts.append(jnp.dot(inputs, columns, preferred_element_type=jnp.float32))
        gates = [acts[0][:, :128], acts[0][:, 128:], acts[1][:, :128]]
        ups = [acts[1][:, 128:], acts[2][:, :128], acts[2][:, 128:]]
        for s in range(3):
            value = gates[s] / (1.0 + jnp.exp(-gates[s])) * ups[s] * weight
            at = j * hidden + s * 128
            hidden_ref[:, at : at + 128] = value.astype(jnp.bfloat16)
    half = own_ref.shape[0]

    down = jnp.concatenate([ref[...] for ref in down_refs], axis=0)
    result = jnp.dot(hidden_ref[...], down, preferred_element_type=jnp.float32)
    result = result.astype(jnp.bfloat16)
    own_ref[...] = result[:half]
    other_ref[...] = result[half:]


def experts(pieces, w_gate, w_up, *w_down):
    counts = tuple(piece.shape[0] for piece in pieces)
    total = sum(counts)
    local, width, hidden = w_gate.shape
    vmem = pl.BlockSpec(memory_space=pltpu.VMEM)
    held = [pltpu.with_memory_space_constraint(v, pltpu.VMEM) for v in (*pieces, w_gate, w_up, *w_down)]
    return pl.pallas_call(
        functools.partial(expert_kernel, counts, local, width, hidden),
        out_shape=[pltpu.VMEM((total // 2, width), jnp.bfloat16)] * 2,
        in_specs=[vmem] * len(held),
        out_specs=[vmem] * 2,
        scratch_shapes=[
            pltpu.VMEM((total, pieces[0].shape[1]), jnp.bfloat16),
            pltpu.VMEM((total, local * hidden), jnp.bfloat16),
        ],
        compiler_params=pltpu.CompilerParams(vmem_limit_bytes=16 << 20),
        cost_estimate=pl.CostEstimate(
            flops=6 * total * local * hidden * width,
            bytes_accessed=4 * total * width,
            transcendentals=total * local * hidden,
        ),
    )(*held)


def after(values, *others):
    return lax.optimization_barrier((*values, *others))[: len(values)]


def per_device(tokens, expert_ids, route_gates, w_gate, w_up, w_down):
    rows, _ = tokens.shape
    picks = expert_ids.shape[1]
    half = 8 * rows
    spare = jnp.zeros((rows, 128 - 2 * picks), tokens.dtype)
    block = jnp.concatenate([tokens, expert_ids.astype(tokens.dtype), route_gates, spare], axis=1)
    gate, down0 = loaded(w_gate, w_down, 0)
    one = [move(block, -step, 0) for step in (1, 2, 3)]
    up, down1 = loaded(w_up, w_down, 1)
    weights = (gate, up, down0, down1)
    block = jnp.concatenate([block] + one, axis=0)
    two = [move(block, -step, 1) for step in (1, 2, 3)]
    near_a = jnp.concatenate([block, two[0]], axis=0)
    near_b = jnp.concatenate([two[1], two[2]], axis=0)
    ahead_a = move(near_a, -1)
    behind_b = move(near_b, 1)

    own0, other0 = experts((near_a, near_b, swap(near_a), swap(near_b)), *weights)
    ahead_a, behind_b = after((ahead_a, behind_b), other0)
    far_a = move(ahead_a, -1)
    far_b = move(behind_b, 1)
    ahead_b = move(near_b, -1)
    behind_a = move(near_a, 1)
    pieces = (ahead_a, behind_b, swap(ahead_a), swap(behind_b))
    own1, other1 = experts(pieces, *weights)
    back1 = swap(other1)

    far_a, far_b = after((far_a, far_b), other1)
    pieces = (far_a, far_b, swap(far_a), swap(far_b))
    own2, other2 = experts(pieces, *weights)
    back2 = swap(other2)
    through_a = move(added(own2[:half], back2[:half]), -1)
    through_b = move(added(own2[half:], back2[half:]), 1)
    got_a = move(added(own1[:half], back1[:half]), 1)
    got_b = move(added(own1[half:], back1[half:]), -1)

    ahead_b, behind_a = after((ahead_b, behind_a), other2)
    pieces = (ahead_b, behind_a, swap(ahead_b), swap(behind_a))
    own3, other3 = experts(pieces, *weights)
    sum3 = added(own3, swap(other3))
    more_b = move(added(sum3[:half], through_b), 1)
    more_a = move(added(sum3[half:], through_a), -1)
    sum0 = added(own0, swap(other0))
    quarter = half // 2
    parts = []
    for side, got, more in ((sum0[:half], got_a, more_a), (sum0[half:], got_b, more_b)):
        for at in (0, quarter):
            parts.append(added(*[v[at : at + quarter] for v in (side, got, more)]))
    for phase in (1, 0):
        arrived = [move(parts[step], step, phase) for step in (1, 2, 3)]
        block = added(parts[0], *arrived)
        parts = [block[step * rows : (step + 1) * rows] for step in range(4)]
    return block


def solution(mesh):
    placed = (
        P(AXES, None),
        P(AXES, None),
        P(AXES, None),
        P("expert", None, "attn"),
        P("expert", None, "attn"),
        P("expert", "attn", None),
    )

    return jax.shard_map(
        per_device, mesh=mesh, in_specs=placed, out_specs=P(AXES, None), check_vma=False
    )
```
